128 devices in a mesh: kpt: 4 (over x, y), row: 16 (over z), col: 2 (over core).
Axes of the slice: x: 2, y: 2, z: 16, core: 2. Of those that a mesh axis runs over, the one named last changes fastest.
The devices are a block of a 8x8x16 slice.
Arguments:
- wannier: float32 [128, 32, 1024], P('kpt', ('row', 'col')), parts along dimension 0, may hold values from -6 to 6
- pairs: int32 [384, 2], replicated, may hold values from 0 to 31, as said below
- gmap: int32 [8192], replicated, may hold values from 1 to 32767, as said below
- screened: bfloat16 [8, 2, 8192, 8192], P('kpt', None, 'row', 'col'), parts along dimension 0, may hold values from -0.046875 to 0.046875
Outputs:
- coulomb: float32 [2, 2, 1536, 384], P(None, None, ('kpt', 'row', 'col')), parts along dimension 2
The draws below stay inside these ranges and needn't reach their ends.
There are 4 independent parts, one for each index of `kpt`. The reference program is written for one: setup_inputs(seed, part) draws one part's arguments, and reference() takes and returns one part's arrays. A program takes and returns all parts, laid end to end along the dimension named above; an argument that names none is the same for every part. Nothing has to cross between parts.
Inputs may be any that keep to these rules, and one draw needn't show every extreme that they name: `gmap`: 8192 distinct flat cells of the grid; cell 0 is never among them. `pairs`: in each row the first Wannier function is no greater than the second; no two rows are equal.
All inputs are finite; a program needn't handle non-finite values.
Results may differ from the reference program's by a relative error of at most 0.0082.
Values may be sent and summed in bfloat16 or wider, within the bound.
A program may use at most 128 MiB of HBM per device.

```python
import jax
import jax.numpy as jnp
from jax import lax

NW = 32
GX = 32
NG = 8192
NF = 2
NP = 384
GYZ = 1024


def draw_gmap(key, part):
    order = jax.random.permutation(key, GX * GX * GX - 1)
    return (order[:NG] + 1).astype(jnp.int32)


def draw_pairs(key, part):
    upper = jnp.triu_indices(NW)
    first_all = jnp.asarray(upper[0]).astype(jnp.int32)
    second_all = jnp.asarray(upper[1]).astype(jnp.int32)
    order = jax.random.permutation(jax.random.fold_in(key, 17), first_all.shape[0])
    chosen = order[:NP]
    return jnp.stack([first_all[chosen], second_all[chosen]], axis=1).astype(jnp.int32)


def block_scale(stream_key, dims, pieces, low, largest):
    level, own = 1.0, jax.random.fold_in(stream_key, 6)
    for position, blocks in pieces:
        draws = jnp.exp(jax.random.uniform(jax.random.fold_in(own, position), (blocks,), jnp.float32, low / len(pieces), largest / len(pieces)))
        level = level * jnp.repeat(draws, dims[position] // blocks).reshape([-1 if axis == position else 1 for axis in range(len(dims))])
    return level


def gaussian(own_key, shape, width, most, shards=(), dtype=jnp.bfloat16):
    values = width * jax.random.normal(own_key, shape, jnp.float32)
    if shards:
        values = values * block_scale(own_key, shape, shards, -0.22, 0.18)
    return jnp.clip(values, -most, most).astype(dtype)


def setup_inputs(seed: int = 0, part: int = 0) -> dict:
    streams_of = jax.random.split(jax.random.key(seed), 5)
    part_splits = jax.random.split(jax.random.fold_in(streams_of[4], part), 5)
    wannier = gaussian(part_splits[0], (NW, GX, GYZ), 1.0, 6.0, ((1, 32),), jnp.float32)
    pairs = draw_pairs(jax.random.fold_in(streams_of[4], 71), part)
    gmap = draw_gmap(jax.random.fold_in(streams_of[4], 71), part)
    screened = gaussian(part_splits[3], (NF, 2, NG, NG), (2 * NG) ** -0.5, 0.046875, ((2, 16), (3, 2)))
    return dict(wannier=wannier, pairs=pairs, gmap=gmap, screened=screened)


def reference(wannier, pairs, gmap, screened):
    grid = wannier.reshape(NW, GX, GX, GX)
    density = grid[pairs[:, 0]] * grid[pairs[:, 1]]
    spectrum = jnp.fft.fftn(density, axes=(1, 2, 3), norm='ortho').reshape(NP, GX * GX * GX)
    chosen = jnp.take(spectrum, gmap, axis=1)
    rho_real = jnp.real(chosen).astype(jnp.bfloat16)
    rho_imag = jnp.imag(chosen).astype(jnp.bfloat16)
    left_real = rho_real.astype(jnp.float32)
    left_imag = rho_imag.astype(jnp.float32)
    highest = lax.Precision.HIGHEST
    results = []
    for frequency in range(NF):
        w_real = screened[frequency, 0]
        w_imag = screened[frequency, 1]
        mixed_real = jnp.dot(w_real, rho_real.T, preferred_element_type=jnp.float32) - jnp.dot(w_imag, rho_imag.T, preferred_element_type=jnp.float32)
        mixed_imag = jnp.dot(w_real, rho_imag.T, preferred_element_type=jnp.float32) + jnp.dot(w_imag, rho_real.T, preferred_element_type=jnp.float32)
        u_real = jnp.dot(left_real, mixed_real, precision=highest) + jnp.dot(left_imag, mixed_imag, precision=highest)
        u_imag = jnp.dot(left_real, mixed_imag, precision=highest) - jnp.dot(left_imag, mixed_real, precision=highest)
        results.append(jnp.stack([u_real, u_imag], axis=0))
    return jnp.stack(results, axis=0) / jnp.sqrt(jnp.float32(NG))
```

```python
import functools
import math

import jax
import jax.numpy as jnp
from jax import lax
from jax.experimental import pallas as pl
from jax.experimental.pallas import tpu as pltpu
from jax.sharding import PartitionSpec as P

MESH = pl.DeviceIdType.MESH
GX = 32
F32 = jnp.float32
BF16 = jnp.bfloat16


def dot(a, b):
    return lax.dot_general(a, b, (((1,), (0,)), ((), ())), preferred_element_type=F32)


def dot_tn(a, b):
    return lax.dot_general(a, b, (((0,), (0,)), ((), ())), preferred_element_type=F32)


def greet(targets):
    barrier = pltpu.get_barrier_semaphore()
    for target in targets:
        pl.semaphore_signal(barrier, inc=1, device_id=target, device_id_type=MESH)
    pl.semaphore_wait(barrier, len(targets))


class Ring:
    def __init__(self, n, own_ref, slot_ref, send_sems, recv_sems):
        self.n, self.half = n, n // 2
        self.own, self.slot = own_ref, slot_ref
        self.send_sems, self.recv_sems = send_sems, recv_sems
        self.me = lax.axis_index("row")
        self.rows = own_ref.shape[0] // 2

    def owner(self, way, step):
        return lax.rem(self.me + step + self.n, self.n) if way else lax.rem(self.me - step + self.n, self.n)

    def copy(self, way, chunk, step, first, arriving=False):
        span = pl.ds(chunk * self.rows, self.rows)
        place = self.slot(self.owner(way, step + 1 if arriving else step)).at[span]
        source = self.own.at[span] if first else place
        target = self.owner(way, -1)
        return pltpu.make_async_remote_copy(
            src_ref=source,
            dst_ref=place,
            send_sem=self.send_sems.at[way, chunk, step],
            recv_sem=self.recv_sems.at[way, chunk, step],
            device_id={"row": self.owner(1 - way, 1)},
            device_id_type=MESH,
        )

    def run(self, on_block, before=None):
        last = self.half - 1
        for way in range(2):
            for chunk in range(2):
                self.copy(way, chunk, 0, True).start()
        if before is not None:
            before()

        def step_body(step, _):
            for chunk in range(2):
                for way in range(2):
                    self.copy(way, chunk, step - 1, False, True).wait_recv()
                    self.copy(way, chunk, step, False).start()
            on_block(self.owner(0, step))
            on_block(self.owner(1, step))
            return 0

        lax.fori_loop(1, last, step_body, 0)
        for chunk in range(2):
            for way in range(2):
                self.copy(way, chunk, last - 1, False, True).wait_recv()
                if way == chunk:
                    self.copy(way, chunk, last, False).start()
        on_block(self.owner(0, last))
        on_block(self.owner(1, last))
        for way in range(2):
            self.copy(way, way, last, False, True).wait_recv()
        on_block(self.owner(0, self.half))

    def drain(self):
        for way in range(2):
            for chunk in range(2):
                self.copy(way, chunk, 0, True).wait_send()

        def body(step, _):
            for way in range(2):
                for chunk in range(2):
                    self.copy(way, chunk, step, False).wait_send()
            return 0

        lax.fori_loop(1, self.half - 1, body, 0)
        for way in range(2):
            self.copy(way, way, self.half - 1, False).wait_send()


def neighbours(n, cols):
    row, col = lax.axis_index("row"), lax.axis_index("col")
    right, left = lax.rem(row + 1, n), lax.rem(row + n - 1, n)
    return [{"row": right}, {"row": left}, {"col": 1 - col}]


def planes_kernel(n, own_ref, out_ref, send_sems, recv_sems, pair_send, pair_recv):
    row, col = lax.axis_index("row"), lax.axis_index("col")
    greet(neighbours(n, 2))

    def slot(owner):
        return out_ref.at[owner * 2 + col]

    def pair_copy(source, owner, to_col):
        return pltpu.make_async_remote_copy(
            src_ref=source,
            dst_ref=out_ref.at[owner * 2 + to_col],
            send_sem=pair_send.at[owner],
            recv_sem=pair_recv.at[owner],
            device_id={"col": 1 - col},
            device_id_type=MESH,
        )

    ring = Ring(n, own_ref, slot, send_sems, recv_sems)

    def before():
        pair_copy(own_ref, row, col).start()
        out_ref[row * 2 + col] = own_ref[...]

    def on_block(owner):
        pair_copy(slot(owner), owner, col).start()

    ring.run(on_block, before)
    ring.drain()

    def finish(owner, _):
        pair_copy(slot(owner), owner, col).wait_send()
        pair_copy(slot(owner), owner, 1 - col).wait_recv()
        return 0

    lax.fori_loop(0, n, finish, 0)


def wave_kernel(pair_tiles, w_ref, pick_ref, cos_ref, sin_ref, turn_ref, out_ref, even0, odd0, even1, odd1, acc_re, acc_im):
    side = w_ref.shape[0]
    rows = w_ref.shape[1]

    def densities(x, even, odd):
        plane = w_ref[x].astype(F32)
        for tile in range(pair_tiles):
            columns = pl.ds(tile * 128, 128)
            products = []
            for part in range(4):
                values = []
                for which in range(2):
                    lanes = jnp.broadcast_to(pick_ref[pl.ds(which * pair_tiles + tile, 1), :] + part * 32, plane.shape)
                    values.append(jnp.take_along_axis(plane, lanes, axis=1, mode="promise_in_bounds"))
                products.append(values[0] * values[1])
            for part in range(2):
                span = pl.ds(part * rows, rows)
                even[span, columns] = (products[part] + products[part + 2]).astype(BF16)
                odd[span, columns] = (products[part] - products[part + 2]).astype(BF16)

    def horner(even, odd):
        real = dot(cos_ref[...], even[...])
        imag = dot(sin_ref[...], odd[...])
        for tile in range(pair_tiles):
            columns = pl.ds(tile * 128, 128)
            lanes = slice(tile * 128, tile * 128 + 128)
            old_re, old_im = acc_re[:, columns], acc_im[:, columns]
            acc_re[:, columns] = old_re * turn_ref[0] - old_im * turn_ref[1] + real[:, lanes]
            acc_im[:, columns] = old_re * turn_ref[1] + old_im * turn_ref[0] + imag[:, lanes]

    acc_re[...] = jnp.zeros_like(acc_re)
    acc_im[...] = jnp.zeros_like(acc_im)
    densities(side - 1, even0, odd0)

    def body(turn, _):
        x = side - 1 - 2 * turn
        densities(x - 1, even1, odd1)
        horner(even0, odd0)
        densities(jnp.maximum(x - 2, 0), even0, odd0)
        horner(even1, odd1)
        return 0

    lax.fori_loop(0, side // 2, body, 0)
    count = acc_re.shape[0]
    for tile in range(pair_tiles):
        columns = pl.ds(tile * 128, 128)
        real, imag = acc_re[:, columns], acc_im[:, columns]
        out_ref[pl.ds(0, count), columns] = (real * turn_ref[2] - imag * turn_ref[3]).astype(BF16)
        out_ref[pl.ds(count, count), columns] = (real * turn_ref[3] + imag * turn_ref[2]).astype(BF16)


def matrix_kernel(
    n, scale, rho_ref, w_hbm, out_ref, panel, w_vmem, mixed, left, pair_out, pair_in, blocks_out, blocks_in, last_out, last_in,
    w_sems, send_sems, recv_sems, left_send, left_recv, pair_sems, block_send, block_recv, last_sems,
):
    row, col = lax.axis_index("row"), lax.axis_index("col")
    waves, pairs = rho_ref.shape[0] // 2, rho_ref.shape[1]
    span = mixed.shape[1]
    per_row = span // waves
    owner_col = row // (n // 2)
    holds_left = col == owner_col
    base = lax.rem(row, n // 2) * per_row
    loads = [pltpu.make_async_copy(w_hbm.at[f, part], w_vmem.at[f, part], w_sems.at[f, part]) for f in range(2) for part in range(2)]
    for load in loads:
        load.start()
    greet(neighbours(n, 2))

    def left_copy(owner, place):
        return pltpu.make_async_remote_copy(
            src_ref=panel.at[owner],
            dst_ref=left.at[place],
            send_sem=left_send.at[place],
            recv_sem=left_recv.at[place],
            device_id={"col": 1 - col},
            device_id_type=MESH,
        )

    def multiply(owner, fresh=False):
        columns = pl.ds(pl.multiple_of(owner * waves, waves), waves)
        real, imag = panel[owner, pl.ds(0, waves)], panel[owner, pl.ds(waves, waves)]
        first = jnp.concatenate([real, imag], axis=1)
        second = jnp.concatenate([-imag, real], axis=1)

        def one(f, _):
            value = dot(w_vmem[f, 0, :, columns], first) + dot(w_vmem[f, 1, :, columns], second)
            mixed[f] = value if fresh else mixed[f] + value
            return 0

        lax.fori_loop(0, 2, one, 0)

    def on_block(owner):
        @pl.when(holds_left & (owner >= base) & (owner < base + per_row))
        def _():
            left_copy(owner, owner - base).start()

        multiply(owner)

    def before():
        panel[row] = rho_ref[...]

        @pl.when(holds_left & (row >= base) & (row < base + per_row))
        def _():
            left_copy(row, row - base).start()

        for load in loads:
            load.wait()
        multiply(row, True)

    ring = Ring(n, rho_ref, lambda owner: panel.at[owner], send_sems, recv_sems)
    ring.run(on_block, before)
    ring.drain()

    @pl.when(holds_left)
    def _():
        for place in range(per_row):
            left_copy(base + place, place).wait_send()
            left[place] = panel[base + place]

    @pl.when(jnp.logical_not(holds_left))
    def _():
        for place in range(per_row):
            left_copy(base + place, place).wait_recv()

    def elements(f):
        total = None
        for place in range(per_row):
            rows = pl.ds(place * waves, waves)
            real = mixed[f, rows, pl.ds(0, pairs)].astype(BF16)
            imag = mixed[f, rows, pl.ds(pairs, pairs)].astype(BF16)
            one = dot_tn(left[place, pl.ds(0, waves)], jnp.concatenate([real, imag], axis=1))
            two = dot_tn(left[place, pl.ds(waves, waves)], jnp.concatenate([imag, -real], axis=1))
            total = one + two if total is None else total + one + two
        return total * scale

    pair_copy = pltpu.make_async_remote_copy(
        src_ref=pair_out, dst_ref=pair_in, send_sem=pair_sems.at[0], recv_sem=pair_sems.at[1],
        device_id={"col": 1 - col}, device_id_type=MESH,
    )
    pair_out[...] = elements(1 - col).astype(BF16)
    pair_copy.start()
    value = elements(col)
    pair_copy.wait()
    value = value + pair_in[...].astype(F32)
    share = pairs // n
    for chip in range(n):
        rows = slice(chip * share, chip * share + share)
        blocks_out[chip] = jnp.concatenate([value[rows, :pairs], value[rows, pairs:]], axis=0).astype(BF16)

    def block_copy(to_row, from_row, target):
        return pltpu.make_async_remote_copy(
            src_ref=blocks_out.at[to_row],
            dst_ref=blocks_in.at[from_row],
            send_sem=block_send.at[to_row],
            recv_sem=block_recv.at[from_row],
            device_id={"row": target},
            device_id_type=MESH,
        )

    for offset in range(n - 1):
        away = n // 2 + (offset + 1) // 2 * (1 if offset % 2 else -1)
        target = lax.rem(row + away, n)
        block_copy(target, row, target).start()
    total = blocks_out[row].astype(F32)
    for offset in range(n - 1):
        away = 1 + offset // 2 if offset % 2 == 0 else n - 1 - offset // 2
        source = lax.rem(row + away, n)
        block_copy(source, source, source).wait_recv()
        total = total + blocks_in[source].astype(F32)
    for away in range(1, n):
        target = lax.rem(row + away, n)
        block_copy(target, row, target).wait_send()
    part = share // 2
    pieces = [jnp.stack([total[c * part : c * part + part], total[share + c * part : share + c * part + part]]) for c in range(2)]
    is_first = col == 0
    last_out[...] = jnp.where(is_first, pieces[1], pieces[0])
    last_copy = pltpu.make_async_remote_copy(
        src_ref=last_out, dst_ref=last_in, send_sem=last_sems.at[0], recv_sem=last_sems.at[1],
        device_id={"col": 1 - col}, device_id_type=MESH,
    )
    last_copy.start()
    out_ref[col] = jnp.where(is_first, pieces[0], pieces[1])
    last_copy.wait()
    out_ref[1 - col] = last_in[...]


VMEM = pl.BlockSpec(memory_space=pltpu.VMEM)
DMA = pltpu.SemaphoreType.DMA


def shards(n, wannier, pairs, gmap, screened):
    members, planes, cells = wannier.shape
    count = pairs.shape[0]
    tiles = count // 128
    depth = cells // 4
    quarters = wannier.reshape(members, 4, depth)
    flipped = jnp.flip(quarters[:, 2:], axis=(1, 2))
    plane = jnp.concatenate([quarters[:, :2], flipped], axis=1).transpose(2, 1, 0).reshape(depth, 4 * members).astype(BF16)

    halves = n // 2
    gathered = pl.pallas_call(
        functools.partial(planes_kernel, n),
        out_shape=jax.ShapeDtypeStruct((2 * n, depth, 4 * members), BF16),
        in_specs=[VMEM],
        out_specs=VMEM,
        scratch_shapes=[DMA((2, 2, halves)), DMA((2, 2, halves)), DMA((n,)), DMA((n,))],
        compiler_params=pltpu.CompilerParams(collective_id=0, has_side_effects=True),
        name="planes",
    )(plane)

    waves = gmap.shape[0] // (2 * n)
    start = (lax.axis_index("col") * n + lax.axis_index("row")) * waves
    cell = lax.dynamic_slice_in_dim(gmap, start, waves)
    kx, ky, kz = cell // (GX * GX), cell // GX % GX, cell % GX
    half = jnp.arange(cells // 2, dtype=jnp.int32)
    steps = (ky[:, None] * (2 * (half // GX) + 1) + kz[:, None] * (2 * (half % GX) + 1)) % (2 * GX)
    angles = steps.astype(F32) * (math.pi / GX)
    cosine, sine = jnp.cos(angles).astype(BF16), (-jnp.sin(angles)).astype(BF16)
    turn = kx.astype(F32) * (-2.0 * math.pi / GX)
    shift = ((ky + kz) % (2 * GX)).astype(F32) * (math.pi / GX)
    norm = 1.0 / math.sqrt(GX * GX * GX)
    turns = jnp.stack([jnp.cos(turn), jnp.sin(turn), jnp.cos(shift) * norm, jnp.sin(shift) * norm])
    turns = jnp.broadcast_to(turns[:, :, None], (4, waves, 128))
    picks = pairs.T.reshape(2 * tiles, 128)

    work = 2 * 2 * waves * cells // 2 * count * 2 * n
    rho = pl.pallas_call(
        functools.partial(wave_kernel, tiles),
        out_shape=jax.ShapeDtypeStruct((2 * waves, count), BF16),
        in_specs=[VMEM] * 5,
        out_specs=VMEM,
        scratch_shapes=[pltpu.VMEM((cells // 2, count), BF16)] * 4 + [pltpu.VMEM((waves, count), F32)] * 2,
        cost_estimate=pl.CostEstimate(flops=work, bytes_accessed=4 << 20, transcendentals=0),
        name="waves",
    )(gathered, picks, cosine, sine, turns)

    freqs, _, row_span, col_span = screened.shape
    share = count // n
    return pl.pallas_call(
        functools.partial(matrix_kernel, n, 1.0 / math.sqrt(gmap.shape[0])),
        out_shape=jax.ShapeDtypeStruct((freqs, 2, share // 2, count), F32),
        in_specs=[VMEM, pl.BlockSpec(memory_space=pl.ANY)],
        out_specs=VMEM,
        scratch_shapes=[
            pltpu.VMEM((n, 2 * waves, count), BF16),
            pltpu.VMEM(screened.shape, BF16),
            pltpu.VMEM((freqs, row_span, 2 * count), F32),
            pltpu.VMEM((row_span // waves, 2 * waves, count), BF16),
            pltpu.VMEM((count, 2 * count), BF16),
            pltpu.VMEM((count, 2 * count), BF16),
            pltpu.VMEM((n, 2 * share, count), BF16),
            pltpu.VMEM((n, 2 * share, count), BF16),
            pltpu.VMEM((2, share // 2, count), F32),
            pltpu.VMEM((2, share // 2, count), F32),
            DMA((2, 2)),
            DMA((2, 2, halves)),
            DMA((2, 2, halves)),
            DMA((row_span // waves,)),
            DMA((row_span // waves,)),
            DMA((2,)),
            DMA((n,)),
            DMA((n,)),
            DMA((2,)),
        ],
        compiler_params=pltpu.CompilerParams(collective_id=1, has_side_effects=True, vmem_limit_bytes=60 << 20),
        name="matrix",
    )(rho, screened)


def solution(mesh):
    return jax.shard_map(
        functools.partial(shards, mesh.shape["row"]),
        mesh=mesh,
        in_specs=(P("kpt", ("row", "col"), None), P(), P(), P("kpt", None, "row", "col")),
        out_specs=P(None, None, ("kpt", "row", "col"), None),
        check_vma=False,
    )
```

```python
import functools
import math

import jax
import jax.numpy as jnp
from jax import lax
from jax.experimental import pallas as pl
from jax.experimental.pallas import tpu as pltpu
from jax.sharding import PartitionSpec as P

MESH = pl.DeviceIdType.MESH
GX = 32
F32 = jnp.float32
BF16 = jnp.bfloat16


def dot(a, b):
    return lax.dot_general(a, b, (((1,), (0,)), ((), ())), preferred_element_type=F32)


def dot_tn(a, b):
    return lax.dot_general(a, b, (((0,), (0,)), ((), ())), preferred_element_type=F32)


def greet(targets):
    barrier = pltpu.get_barrier_semaphore()
    for target in targets:
        pl.semaphore_signal(barrier, inc=1, device_id=target, device_id_type=MESH)
    pl.semaphore_wait(barrier, len(targets))


class Ring:
    def __init__(self, n, own_ref, slot_ref, send_sems, recv_sems):
        self.n, self.half = n, n // 2
        self.own, self.slot = own_ref, slot_ref
        self.send_sems, self.recv_sems = send_sems, recv_sems
        self.me = lax.axis_index("row")
        self.rows = own_ref.shape[0] // 2

    def owner(self, way, step):
        return lax.rem(self.me + step + self.n, self.n) if way else lax.rem(self.me - step + self.n, self.n)

    def copy(self, way, chunk, step, first, arriving=False):
        span = pl.ds(chunk * self.rows, self.rows)
        place = self.slot(self.owner(way, step + 1 if arriving else step)).at[span]
        source = self.own.at[span] if first else place
        target = self.owner(way, -1)
        return pltpu.make_async_remote_copy(
            src_ref=source,
            dst_ref=place,
            send_sem=self.send_sems.at[way, chunk, step],
            recv_sem=self.recv_sems.at[way, chunk, step],
            device_id={"row": self.owner(1 - way, 1)},
            device_id_type=MESH,
        )

    def run(self, on_block, before=None):
        last = self.half - 1
        for way in range(2):
            for chunk in range(2):
                self.copy(way, chunk, 0, True).start()
        if before is not None:
            before()

        def step_body(step, _):
            for chunk in range(2):
                for way in range(2):
                    self.copy(way, chunk, step - 1, False, True).wait_recv()
                    self.copy(way, chunk, step, False).start()
            on_block(self.owner(0, step))
            on_block(self.owner(1, step))
            return 0

        lax.fori_loop(1, last, step_body, 0)
        for chunk in range(2):
            for way in range(2):
                self.copy(way, chunk, last - 1, False, True).wait_recv()
                if way == chunk:
                    self.copy(way, chunk, last, False).start()
        on_block(self.owner(0, last))
        on_block(self.owner(1, last))
        for way in range(2):
            self.copy(way, way, last, False, True).wait_recv()
        on_block(self.owner(0, self.half))

    def drain(self):
        for way in range(2):
            for chunk in range(2):
                self.copy(way, chunk, 0, True).wait_send()

        def body(step, _):
            for way in range(2):
                for chunk in range(2):
                    self.copy(way, chunk, step, False).wait_send()
            return 0

        lax.fori_loop(1, self.half - 1, body, 0)
        for way in range(2):
            self.copy(way, way, self.half - 1, False).wait_send()


def neighbours(n, cols):
    row, col = lax.axis_index("row"), lax.axis_index("col")
    right, left = lax.rem(row + 1, n), lax.rem(row + n - 1, n)
    return [{"row": right}, {"row": left}, {"col": 1 - col}]


def pick_lanes(values, lanes):
    numbers = lax.GatherDimensionNumbers(
        offset_dims=(), collapsed_slice_dims=(1,), start_index_map=(1,), operand_batching_dims=(0,), start_indices_batching_dims=(0,)
    )
    return lax.gather(values, lanes[:, :, None], numbers, (1, 1), mode=lax.GatherScatterMode.PROMISE_IN_BOUNDS)


def wave_kernel(
    n, own_ref, pick_ref, cell_ref, out_ref, planes, cosine, sine, turn, power, even0, odd0, even1, odd1, acc_re, acc_im,
    send_sems, recv_sems, pair_send, pair_recv,
):
    row, col = lax.axis_index("row"), lax.axis_index("col")
    depth = own_ref.shape[0]
    waves, pairs = acc_re.shape
    tiles = pairs // 128
    piece = 64
    greet(neighbours(n, 2))

    def slot(owner, which):
        return planes.at[owner * 2 + which]

    def pair_copy(source, owner, to_col):
        return pltpu.make_async_remote_copy(
            src_ref=source,
            dst_ref=slot(owner, to_col),
            send_sem=pair_send.at[owner],
            recv_sem=pair_recv.at[owner],
            device_id={"col": 1 - col},
            device_id_type=MESH,
        )

    def fold(owner, tile, even, odd):
        for which in range(2):
            columns = pl.ds(pl.multiple_of(tile * 256 + which * 128, 128), 128)
            for begin in range(0, depth, piece):
                plane = planes[owner * 2 + which, pl.ds(begin, piece)].astype(F32)
                for part in range(2):
                    values = []
                    for quarter in (part, part + 2):
                        for side in range(2):
                            lanes = pick_ref[pl.ds(side * tiles + tile, 1), :] + quarter * 32
                            values.append(pick_lanes(plane, jnp.broadcast_to(lanes, plane.shape)))
                    one, two = values[0] * values[1], values[2] * values[3]
                    span = pl.ds(part * depth + begin, piece)
                    even[span, columns] = (one + two).astype(BF16)
                    odd[span, columns] = (one - two).astype(BF16)

    def gather(tile, even, odd, sign):
        columns = pl.ds(pl.multiple_of(tile * 128, 128), 128)
        block = pl.ds(pl.multiple_of(tile * 256, 256), 256)
        real = dot(cosine[...], even[:, block])
        imag = dot(sine[...], odd[:, block])
        p_re, p_im = power[0], power[1] * sign
        q_re, q_im = p_re * turn[0] - p_im * turn[1], p_re * turn[1] + p_im * turn[0]
        acc_re[:, columns] += p_re * real[:, :128] - p_im * imag[:, :128] + (q_re * real[:, 128:] - q_im * imag[:, 128:])
        acc_im[:, columns] += p_re * imag[:, :128] + p_im * real[:, :128] + (q_re * imag[:, 128:] + q_im * real[:, 128:])

    def tables():
        lane = lax.broadcasted_iota(jnp.int32, (8, 128), 1)
        angle = (lane & (2 * GX - 1)).astype(F32) * (math.pi / GX)
        cos_lanes, sin_lanes = jnp.cos(angle), jnp.sin(angle)
        copies = waves // 8

        def look(steps):
            at = steps & (2 * GX - 1)
            return (
                pick_lanes(jnp.concatenate([cos_lanes] * copies, axis=0), at),
                pick_lanes(jnp.concatenate([sin_lanes] * copies, axis=0), at),
            )

        bits = GX.bit_length() - 1
        cell = cell_ref[...]
        kx, ky, kz = cell >> (2 * bits), (cell >> bits) & (GX - 1), cell & (GX - 1)

        def fill(index, _):
            begin = pl.multiple_of(index * 128, 128)
            spot = lax.broadcasted_iota(jnp.int32, cell.shape, 1) + begin
            real, imag = look(ky * (2 * (spot >> bits) + 1) + kz * (2 * (spot & (GX - 1)) + 1))
            cosine[:, pl.ds(begin, 128)] = real.astype(BF16)
            sine[:, pl.ds(begin, 128)] = (-imag).astype(BF16)
            return 0

        lax.fori_loop(0, 2 * depth // 128, fill, 0)
        turn[0], turn[1] = look(kx * -2)
        turn[2], turn[3] = look(kx * -4)
        norm = 1.0 / math.sqrt(GX * GX * GX)
        real, imag = look(ky + kz - kx * 4 * row)
        turn[4], turn[5] = real * norm, imag * norm
        power[0] = jnp.ones(cell.shape, F32)
        power[1] = jnp.zeros(cell.shape, F32)

    def advance():
        p_re, p_im = power[0], power[1]
        power[0] = p_re * turn[2] - p_im * turn[3]
        power[1] = p_re * turn[3] + p_im * turn[2]

    ring = Ring(n, own_ref, lambda owner: slot(owner, col), send_sems, recv_sems)
    half = n // 2

    def arrive(step):
        for chunk in range(2):
            for way in range(2):
                if way == chunk:
                    ring.copy(way, chunk, step - 1, False, True).wait_recv()

                    @pl.when(step < half)
                    def _():
                        ring.copy(way, chunk, step, False).start()
                else:
                    @pl.when(step < half)
                    def _():
                        ring.copy(way, chunk, step - 1, False, True).wait_recv()

                    @pl.when(step < half - 1)
                    def _():
                        ring.copy(way, chunk, step, False).start()
        ahead, behind = ring.owner(1, step), ring.owner(0, step)
        pair_copy(slot(ahead, col), ahead, col).start()

        @pl.when(step < half)
        def _():
            pair_copy(slot(behind, col), behind, col).start()

    def paired(owner):
        pair_copy(own_ref, owner, 1 - col).wait_recv()

    def each_tile(work):
        def one(tile, _):
            work(tile)
            return 0

        lax.fori_loop(0, tiles, one, 0)

    def first_half(owner):
        def work(tile):
            gather(tile, even1, odd1, -1.0)
            fold(owner, tile, even0, odd0)

        each_tile(work)
        advance()

    for way in range(2):
        for chunk in range(2):
            ring.copy(way, chunk, 0, True).start()
    pair_copy(own_ref, row, col).start()
    planes[row * 2 + col] = own_ref[...]
    acc_re[...] = jnp.zeros_like(acc_re)
    acc_im[...] = jnp.zeros_like(acc_im)
    tables()
    arrive(1)
    paired(row)
    each_tile(lambda tile: fold(row, tile, even1, odd1))

    def body(step, _):
        arrive(step)
        ahead, behind = ring.owner(1, step - 1), ring.owner(0, step - 1)
        paired(ahead)
        paired(behind)
        first_half(ahead)

        def work(tile):
            gather(tile, even0, odd0, 1.0)
            fold(behind, tile, even1, odd1)

        each_tile(work)
        return 0

    lax.fori_loop(2, half + 1, body, 0)
    across = ring.owner(0, half)
    paired(across)
    first_half(across)
    each_tile(lambda tile: gather(tile, even0, odd0, 1.0))
    for tile in range(tiles):
        columns = pl.ds(tile * 128, 128)
        real, imag = acc_re[:, columns], acc_im[:, columns]
        out_ref[pl.ds(0, waves), columns] = (real * turn[4] - imag * turn[5]).astype(BF16)
        out_ref[pl.ds(waves, waves), columns] = (real * turn[5] + imag * turn[4]).astype(BF16)
    ring.drain()

    def finish(owner, _):
        pair_copy(own_ref, owner, col).wait_send()
        return 0

    lax.fori_loop(0, n, finish, 0)


def matrix_kernel(
    n, scale, rho_ref, w_hbm, out_ref, panel, w_vmem, mixed, left, pair_out, pair_in, blocks_out, blocks_in, last_out, last_in,
    w_sems, send_sems, recv_sems, left_send, left_recv, pair_sems, block_send, block_recv, last_sems,
):
    row, col = lax.axis_index("row"), lax.axis_index("col")
    waves, pairs = rho_ref.shape[0] // 2, rho_ref.shape[1]
    span = mixed.shape[1]
    per_row = span // waves
    owner_col = row // (n // 2)
    holds_left = col == owner_col
    base = lax.rem(row, n // 2) * per_row
    loads = [pltpu.make_async_copy(w_hbm.at[f, part], w_vmem.at[f, part], w_sems.at[f, part]) for f in range(2) for part in range(2)]
    for load in loads:
        load.start()
    greet(neighbours(n, 2))

    def left_copy(owner, place):
        return pltpu.make_async_remote_copy(
            src_ref=panel.at[owner],
            dst_ref=left.at[place],
            send_sem=left_send.at[place],
            recv_sem=left_recv.at[place],
            device_id={"col": 1 - col},
            device_id_type=MESH,
        )

    def multiply(owner, fresh=False):
        columns = pl.ds(pl.multiple_of(owner * waves, waves), waves)
        real, imag = panel[owner, pl.ds(0, waves)], panel[owner, pl.ds(waves, waves)]
        first = jnp.concatenate([real, imag], axis=1)
        second = jnp.concatenate([-imag, real], axis=1)

        def one(f, _):
            value = dot(w_vmem[f, 0, :, columns], first) + dot(w_vmem[f, 1, :, columns], second)
            mixed[f] = value if fresh else mixed[f] + value
            return 0

        lax.fori_loop(0, 2, one, 0)

    def on_block(owner):
        @pl.when(holds_left & (owner >= base) & (owner < base + per_row))
        def _():
            left_copy(owner, owner - base).start()

        multiply(owner)

    def before():
        panel[row] = rho_ref[...]

        @pl.when(holds_left & (row >= base) & (row < base + per_row))
        def _():
            left_copy(row, row - base).start()

        for load in loads:
            load.wait()
        multiply(row, True)

    ring = Ring(n, rho_ref, lambda owner: panel.at[owner], send_sems, recv_sems)
    ring.run(on_block, before)
    ring.drain()

    @pl.when(holds_left)
    def _():
        for place in range(per_row):
            left_copy(base + place, place).wait_send()
            left[place] = panel[base + place]

    @pl.when(jnp.logical_not(holds_left))
    def _():
        for place in range(per_row):
            left_copy(base + place, place).wait_recv()

    def elements(f):
        total = None
        for place in range(per_row):
            rows = pl.ds(place * waves, waves)
            real = mixed[f, rows, pl.ds(0, pairs)].astype(BF16)
            imag = mixed[f, rows, pl.ds(pairs, pairs)].astype(BF16)
            one = dot_tn(left[place, pl.ds(0, waves)], jnp.concatenate([real, imag], axis=1))
            two = dot_tn(left[place, pl.ds(waves, waves)], jnp.concatenate([imag, -real], axis=1))
            total = one + two if total is None else total + one + two
        return total * scale

    pair_copy = pltpu.make_async_remote_copy(
        src_ref=pair_out, dst_ref=pair_in, send_sem=pair_sems.at[0], recv_sem=pair_sems.at[1],
        device_id={"col": 1 - col}, device_id_type=MESH,
    )
    pair_out[...] = elements(1 - col).astype(BF16)
    pair_copy.start()
    value = elements(col)
    pair_copy.wait()
    value = value + pair_in[...].astype(F32)
    share = pairs // n
    for chip in range(n):
        rows = slice(chip * share, chip * share + share)
        blocks_out[chip] = jnp.concatenate([value[rows, :pairs], value[rows, pairs:]], axis=0).astype(BF16)

    def block_copy(to_row, from_row, target):
        return pltpu.make_async_remote_copy(
            src_ref=blocks_out.at[to_row],
            dst_ref=blocks_in.at[from_row],
            send_sem=block_send.at[to_row],
            recv_sem=block_recv.at[from_row],
            device_id={"row": target},
            device_id_type=MESH,
        )

    for offset in range(n - 1):
        away = n // 2 + (offset + 1) // 2 * (1 if offset % 2 else -1)
        target = lax.rem(row + away, n)
        block_copy(target, row, target).start()
    total = blocks_out[row].astype(F32)
    for offset in range(n - 1):
        away = 1 + offset // 2 if offset % 2 == 0 else n - 1 - offset // 2
        source = lax.rem(row + away, n)
        block_copy(source, source, source).wait_recv()
        total = total + blocks_in[source].astype(F32)
    for away in range(1, n):
        target = lax.rem(row + away, n)
        block_copy(target, row, target).wait_send()
    part = share // 2
    pieces = [jnp.stack([total[c * part : c * part + part], total[share + c * part : share + c * part + part]]) for c in range(2)]
    is_first = col == 0
    last_out[...] = jnp.where(is_first, pieces[1], pieces[0])
    last_copy = pltpu.make_async_remote_copy(
        src_ref=last_out, dst_ref=last_in, send_sem=last_sems.at[0], recv_sem=last_sems.at[1],
        device_id={"col": 1 - col}, device_id_type=MESH,
    )
    last_copy.start()
    out_ref[col] = jnp.where(is_first, pieces[0], pieces[1])
    last_copy.wait()
    out_ref[1 - col] = last_in[...]


VMEM = pl.BlockSpec(memory_space=pltpu.VMEM)
DMA = pltpu.SemaphoreType.DMA


def shards(n, wannier, pairs, gmap, screened):
    members, planes, cells = wannier.shape
    count = pairs.shape[0]
    tiles = count // 128
    depth = cells // 4
    quarters = wannier.reshape(members, 4, depth)
    flipped = jnp.flip(quarters[:, 2:], axis=(1, 2))
    plane = jnp.concatenate([quarters[:, :2], flipped], axis=1).transpose(2, 1, 0).reshape(depth, 4 * members).astype(BF16)

    halves = n // 2
    waves = gmap.shape[0] // (2 * n)
    start = (lax.axis_index("col") * n + lax.axis_index("row")) * waves
    cell = jnp.broadcast_to(lax.dynamic_slice_in_dim(gmap, start, waves)[:, None], (waves, 128))
    picks = pairs.T.reshape(2 * tiles, 128)
    rho = pl.pallas_call(
        functools.partial(wave_kernel, n),
        out_shape=jax.ShapeDtypeStruct((2 * waves, count), BF16),
        in_specs=[VMEM] * 3,
        out_specs=VMEM,
        scratch_shapes=[
            pltpu.VMEM((2 * n, depth, 4 * members), BF16),
            pltpu.VMEM((waves, cells // 2), BF16),
            pltpu.VMEM((waves, cells // 2), BF16),
            pltpu.VMEM((6, waves, 128), F32),
            pltpu.VMEM((2, waves, 128), F32),
        ]
        + [pltpu.VMEM((cells // 2, 2 * count), BF16)] * 4
        + [pltpu.VMEM((waves, count), F32)] * 2
        + [DMA((2, 2, halves)), DMA((2, 2, halves)), DMA((n,)), DMA((n,))],
        compiler_params=pltpu.CompilerParams(collective_id=0, has_side_effects=True),
        name="waves",
    )(plane, picks, cell)

    freqs, _, row_span, col_span = screened.shape
    share = count // n
    return pl.pallas_call(
        functools.partial(matrix_kernel, n, 1.0 / math.sqrt(gmap.shape[0])),
        out_shape=jax.ShapeDtypeStruct((freqs, 2, share // 2, count), F32),
        in_specs=[VMEM, pl.BlockSpec(memory_space=pl.ANY)],
        out_specs=VMEM,
        scratch_shapes=[
            pltpu.VMEM((n, 2 * waves, count), BF16),
            pltpu.VMEM(screened.shape, BF16),
            pltpu.VMEM((freqs, row_span, 2 * count), F32),
            pltpu.VMEM((row_span // waves, 2 * waves, count), BF16),
            pltpu.VMEM((count, 2 * count), BF16),
            pltpu.VMEM((count, 2 * count), BF16),
            pltpu.VMEM((n, 2 * share, count), BF16),
            pltpu.VMEM((n, 2 * share, count), BF16),
            pltpu.VMEM((2, share // 2, count), F32),
            pltpu.VMEM((2, share // 2, count), F32),
            DMA((2, 2)),
            DMA((2, 2, halves)),
            DMA((2, 2, halves)),
            DMA((row_span // waves,)),
            DMA((row_span // waves,)),
            DMA((2,)),
            DMA((n,)),
            DMA((n,)),
            DMA((2,)),
        ],
        compiler_params=pltpu.CompilerParams(collective_id=1, has_side_effects=True, vmem_limit_bytes=60 << 20),
        name="matrix",
    )(rho, screened)


def solution(mesh):
    return jax.shard_map(
        functools.partial(shards, mesh.shape["row"]),
        mesh=mesh,
        in_specs=(P("kpt", ("row", "col"), None), P(), P(), P("kpt", None, "row", "col")),
        out_specs=P(None, None, ("kpt", "row", "col"), None),
        check_vma=False,
    )
```

```python
import functools
import math

import jax
import jax.numpy as jnp
from jax import lax
from jax.experimental import pallas as pl
from jax.experimental.pallas import tpu as pltpu
from jax.sharding import PartitionSpec as P

MESH = pl.DeviceIdType.MESH
GX = 32
F32 = jnp.float32
BF16 = jnp.bfloat16


def dot(a, b):
    return lax.dot_general(a, b, (((1,), (0,)), ((), ())), preferred_element_type=F32)


def dot_tn(a, b):
    return lax.dot_general(a, b, (((0,), (0,)), ((), ())), preferred_element_type=F32)


def greet(targets, between=None):
    barrier = pltpu.get_barrier_semaphore()
    for target in targets:
        pl.semaphore_signal(barrier, inc=1, device_id=target, device_id_type=MESH)
    if between is not None:
        between()
    pl.semaphore_wait(barrier, len(targets))


class Ring:
    def __init__(self, n, own_ref, slot_ref, send_sems, recv_sems):
        self.n, self.half = n, n // 2
        self.own, self.slot = own_ref, slot_ref
        self.send_sems, self.recv_sems = send_sems, recv_sems
        self.me = lax.axis_index("row")
        self.rows = own_ref.shape[0] // 2

    def owner(self, way, step):
        return lax.rem(self.me + step + self.n, self.n) if way else lax.rem(self.me - step + self.n, self.n)

    def copy(self, way, chunk, step, first, arriving=False):
        span = pl.ds(chunk * self.rows, self.rows)
        place = self.slot(self.owner(way, step + 1 if arriving else step)).at[span]
        source = self.own.at[span] if first else place
        target = self.owner(way, -1)
        return pltpu.make_async_remote_copy(
            src_ref=source,
            dst_ref=place,
            send_sem=self.send_sems.at[way, chunk, step],
            recv_sem=self.recv_sems.at[way, chunk, step],
            device_id={"row": self.owner(1 - way, 1)},
            device_id_type=MESH,
        )

    def run(self, on_block, before=None):
        last = self.half - 1
        for way in range(2):
            for chunk in range(2):
                self.copy(way, chunk, 0, True).start()
        if before is not None:
            before()

        def step_body(step, _):
            for chunk in range(2):
                for way in range(2):
                    self.copy(way, chunk, step - 1, False, True).wait_recv()
                    self.copy(way, chunk, step, False).start()
            on_block(self.owner(0, step))
            on_block(self.owner(1, step))
            return 0

        lax.fori_loop(1, last, step_body, 0)
        for chunk in range(2):
            for way in range(2):
                self.copy(way, chunk, last - 1, False, True).wait_recv()
                if way == chunk:
                    self.copy(way, chunk, last, False).start()
        on_block(self.owner(0, last))
        on_block(self.owner(1, last))
        for way in range(2):
            self.copy(way, way, last, False, True).wait_recv()
        on_block(self.owner(0, self.half))

    def drain(self):
        for way in range(2):
            for chunk in range(2):
                self.copy(way, chunk, 0, True).wait_send()

        def body(step, _):
            for way in range(2):
                for chunk in range(2):
                    self.copy(way, chunk, step, False).wait_send()
            return 0

        lax.fori_loop(1, self.half - 1, body, 0)
        for way in range(2):
            self.copy(way, way, self.half - 1, False).wait_send()


def neighbours(n, cols):
    row, col = lax.axis_index("row"), lax.axis_index("col")
    right, left = lax.rem(row + 1, n), lax.rem(row + n - 1, n)
    return [{"row": right}, {"row": left}, {"col": 1 - col}]


def pick_lanes(values, lanes):
    numbers = lax.GatherDimensionNumbers(
        offset_dims=(), collapsed_slice_dims=(1,), start_index_map=(1,), operand_batching_dims=(0,), start_indices_batching_dims=(0,)
    )
    return lax.gather(values, lanes[:, :, None], numbers, (1, 1), mode=lax.GatherScatterMode.PROMISE_IN_BOUNDS)


def wave_kernel(
    n, wannier_ref, pick_ref, gmap_ref, out_ref, own_ref, cell_ref, planes, cosine, sine, turn, power, even0, odd0, even1, odd1, acc_re, acc_im,
    send_sems, recv_sems, pair_send, pair_recv,
):
    row, col = lax.axis_index("row"), lax.axis_index("col")
    depth = own_ref.shape[0]
    waves, pairs = acc_re.shape
    tiles = pairs // 128
    piece = 64

    def prepare():
        values = wannier_ref[:, 0, :]
        back = 127 - lax.broadcasted_iota(jnp.int32, (values.shape[0], 128), 1)
        parts = [values[:, :depth], values[:, depth : 2 * depth]]
        for quarter in (3, 2):
            tail = [pick_lanes(values[:, quarter * depth + lane : quarter * depth + lane + 128], back) for lane in range(0, depth, 128)]
            parts.append(jnp.concatenate(tail[::-1], axis=1))
        own_ref[...] = jnp.concatenate(parts, axis=0).T.astype(BF16)
        for begin in range(0, waves, 128):
            line = gmap_ref[pl.ds((col * n + row) * (waves // 128) + begin // 128, 1), :].astype(F32)
            cell_ref[pl.ds(begin, 128)] = jnp.broadcast_to(line, (128, 128)).T.astype(jnp.int32)

    greet(neighbours(n, 2), prepare)

    def slot(owner, which):
        return planes.at[owner * 2 + which]

    def pair_copy(source, owner, to_col):
        return pltpu.make_async_remote_copy(
            src_ref=source,
            dst_ref=slot(owner, to_col),
            send_sem=pair_send.at[owner],
            recv_sem=pair_recv.at[owner],
            device_id={"col": 1 - col},
            device_id_type=MESH,
        )

    def fold(owner, tile, even, odd):
        for which in range(2):
            columns = pl.ds(pl.multiple_of(tile * 256 + which * 128, 128), 128)
            for begin in range(0, depth, piece):
                plane = planes[owner * 2 + which, pl.ds(begin, piece)].astype(F32)
                for part in range(2):
                    values = []
                    for quarter in (part, part + 2):
                        for side in range(2):
                            lanes = pick_ref[pl.ds(side, 1), pl.ds(pl.multiple_of(tile * 128, 128), 128)] + quarter * 32
                            values.append(pick_lanes(plane, jnp.broadcast_to(lanes, plane.shape)))
                    one, two = values[0] * values[1], values[2] * values[3]
                    span = pl.ds(part * depth + begin, piece)
                    even[span, columns] = (one + two).astype(BF16)
                    odd[span, columns] = (one - two).astype(BF16)

    def gather(tile, even, odd, sign):
        columns = pl.ds(pl.multiple_of(tile * 128, 128), 128)
        block = pl.ds(pl.multiple_of(tile * 256, 256), 256)
        real = dot(cosine[...], even[:, block])
        imag = dot(sine[...], odd[:, block])
        p_re, p_im = power[0], power[1] * sign
        at = 2 if sign > 0 else 4
        q_re, q_im = power[at], power[at + 1]
        acc_re[:, columns] += p_re * real[:, :128] - p_im * imag[:, :128] + (q_re * real[:, 128:] - q_im * imag[:, 128:])
        acc_im[:, columns] += p_re * imag[:, :128] + p_im * real[:, :128] + (q_re * imag[:, 128:] + q_im * real[:, 128:])

    def set_power(p_re, p_im):
        power[0], power[1] = p_re, p_im
        one, two = p_re * turn[0], p_im * turn[1]
        three, four = p_re * turn[1], p_im * turn[0]
        power[2], power[3] = one - two, three + four
        power[4], power[5] = one + two, three - four

    def tables():
        lane = lax.broadcasted_iota(jnp.int32, (8, 128), 1)
        angle = (lane & (2 * GX - 1)).astype(F32) * (math.pi / GX)
        cos_lanes, sin_lanes = jnp.cos(angle), jnp.sin(angle)
        copies = waves // 8

        def look(steps):
            at = steps & (2 * GX - 1)
            return (
                pick_lanes(jnp.concatenate([cos_lanes] * copies, axis=0), at),
                pick_lanes(jnp.concatenate([sin_lanes] * copies, axis=0), at),
            )

        bits = GX.bit_length() - 1
        cell = cell_ref[...]
        kx, ky, kz = cell >> (2 * bits), (cell >> bits) & (GX - 1), cell & (GX - 1)

        def fill(index, _):
            begin = pl.multiple_of(index * 128, 128)
            spot = lax.broadcasted_iota(jnp.int32, cell.shape, 1) + begin
            real, imag = look(ky * (2 * (spot >> bits) + 1) + kz * (2 * (spot & (GX - 1)) + 1))
            cosine[:, pl.ds(begin, 128)] = real.astype(BF16)
            sine[:, pl.ds(begin, 128)] = (-imag).astype(BF16)
            return 0

        lax.fori_loop(0, 2 * depth // 128, fill, 0)
        turn[0], turn[1] = look(kx * -2)
        turn[2], turn[3] = look(kx * -4)
        norm = 1.0 / math.sqrt(GX * GX * GX)
        real, imag = look(ky + kz - kx * 4 * row)
        turn[4], turn[5] = real * norm, imag * norm
        set_power(jnp.ones(cell.shape, F32), jnp.zeros(cell.shape, F32))

    def advance():
        p_re, p_im = power[0], power[1]
        set_power(p_re * turn[2] - p_im * turn[3], p_re * turn[3] + p_im * turn[2])

    ring = Ring(n, own_ref, lambda owner: slot(owner, col), send_sems, recv_sems)
    half = n // 2

    def arrive(step):
        for chunk in range(2):
            for way in range(2):
                if way == chunk:
                    ring.copy(way, chunk, step - 1, False, True).wait_recv()

                    @pl.when(step < half)
                    def _():
                        ring.copy(way, chunk, step, False).start()
                else:
                    @pl.when(step < half)
                    def _():
                        ring.copy(way, chunk, step - 1, False, True).wait_recv()

                    @pl.when(step < half - 1)
                    def _():
                        ring.copy(way, chunk, step, False).start()
        ahead, behind = ring.owner(1, step), ring.owner(0, step)
        pair_copy(slot(ahead, col), ahead, col).start()

        @pl.when(step < half)
        def _():
            pair_copy(slot(behind, col), behind, col).start()

    def paired(owner):
        pair_copy(own_ref, owner, 1 - col).wait_recv()

    def each_tile(work):
        def one(tile, _):
            work(tile)
            return 0

        lax.fori_loop(0, tiles, one, 0)

    def first_half(owner):
        def work(tile):
            gather(tile, even1, odd1, -1.0)
            fold(owner, tile, even0, odd0)

        each_tile(work)
        advance()

    for way in range(2):
        for chunk in range(2):
            ring.copy(way, chunk, 0, True).start()
    pair_copy(own_ref, row, col).start()
    planes[row * 2 + col] = own_ref[...]
    acc_re[...] = jnp.zeros_like(acc_re)
    acc_im[...] = jnp.zeros_like(acc_im)
    tables()
    arrive(1)
    paired(row)
    each_tile(lambda tile: fold(row, tile, even1, odd1))

    def body(step, _):
        arrive(step)
        ahead, behind = ring.owner(1, step - 1), ring.owner(0, step - 1)
        paired(ahead)
        paired(behind)
        first_half(ahead)

        def work(tile):
            gather(tile, even0, odd0, 1.0)
            fold(behind, tile, even1, odd1)

        each_tile(work)
        return 0

    lax.fori_loop(2, half + 1, body, 0)
    across = ring.owner(0, half)
    paired(across)
    first_half(across)
    each_tile(lambda tile: gather(tile, even0, odd0, 1.0))
    for tile in range(tiles):
        columns = pl.ds(tile * 128, 128)
        real, imag = acc_re[:, columns], acc_im[:, columns]
        out_ref[pl.ds(0, waves), columns] = (real * turn[4] - imag * turn[5]).astype(BF16)
        out_ref[pl.ds(waves, waves), columns] = (real * turn[5] + imag * turn[4]).astype(BF16)
    ring.drain()

    def finish(owner, _):
        pair_copy(own_ref, owner, col).wait_send()
        return 0

    lax.fori_loop(0, n, finish, 0)


def matrix_kernel(
    n, scale, rho_ref, w_hbm, out_ref, panel, w_vmem, mixed, left, pair_out, pair_in, own_sums, near_out, near_in,
    far_out, far_in, last_out, last_in, w_sems, send_sems, recv_sems, left_send, left_recv, pair_sems, near_send, near_recv,
    far_send, far_recv, last_sems,
):
    row, col = lax.axis_index("row"), lax.axis_index("col")
    waves, pairs = rho_ref.shape[0] // 2, rho_ref.shape[1]
    span = mixed.shape[1]
    per_row = span // waves
    owner_col = row // (n // 2)
    holds_left = col == owner_col
    base = lax.rem(row, n // 2) * per_row
    loads = [pltpu.make_async_copy(w_hbm.at[f, part], w_vmem.at[f, part], w_sems.at[f, part]) for f in range(2) for part in range(2)]
    for load in loads:
        load.start()
    greet(neighbours(n, 2))

    def left_copy(owner, place):
        return pltpu.make_async_remote_copy(
            src_ref=panel.at[owner],
            dst_ref=left.at[place],
            send_sem=left_send.at[place],
            recv_sem=left_recv.at[place],
            device_id={"col": 1 - col},
            device_id_type=MESH,
        )

    def multiply(owner, fresh=False):
        columns = pl.ds(pl.multiple_of(owner * waves, waves), waves)
        real, imag = panel[owner, pl.ds(0, waves)], panel[owner, pl.ds(waves, waves)]
        first = jnp.concatenate([real, imag], axis=1)
        second = jnp.concatenate([-imag, real], axis=1)

        def one(f, _):
            value = dot(w_vmem[f, 0, :, columns], first) + dot(w_vmem[f, 1, :, columns], second)
            mixed[f] = value if fresh else mixed[f] + value
            return 0

        lax.fori_loop(0, 2, one, 0)

    def on_block(owner):
        @pl.when(holds_left & (owner >= base) & (owner < base + per_row))
        def _():
            left_copy(owner, owner - base).start()

        multiply(owner)

    def before():
        panel[row] = rho_ref[...]

        @pl.when(holds_left & (row >= base) & (row < base + per_row))
        def _():
            left_copy(row, row - base).start()

        for load in loads:
            load.wait()
        multiply(row, True)

    ring = Ring(n, rho_ref, lambda owner: panel.at[owner], send_sems, recv_sems)
    ring.run(on_block, before)
    ring.drain()

    @pl.when(holds_left)
    def _():
        for place in range(per_row):
            left_copy(base + place, place).wait_send()
            left[place] = panel[base + place]

    @pl.when(jnp.logical_not(holds_left))
    def _():
        for place in range(per_row):
            left_copy(base + place, place).wait_recv()

    def elements(f):
        total = None
        for place in range(per_row):
            rows = pl.ds(place * waves, waves)
            real = mixed[f, rows, pl.ds(0, pairs)].astype(BF16)
            imag = mixed[f, rows, pl.ds(pairs, pairs)].astype(BF16)
            one = dot_tn(left[place, pl.ds(0, waves)], jnp.concatenate([real, imag], axis=1))
            two = dot_tn(left[place, pl.ds(waves, waves)], jnp.concatenate([imag, -real], axis=1))
            total = one + two if total is None else total + one + two
        return total * scale

    pair_copy = pltpu.make_async_remote_copy(
        src_ref=pair_out, dst_ref=pair_in, send_sem=pair_sems.at[0], recv_sem=pair_sems.at[1],
        device_id={"col": 1 - col}, device_id_type=MESH,
    )
    pair_out[...] = elements(1 - col).astype(BF16)
    pair_copy.start()
    value = elements(col)
    pair_copy.wait()
    value = value + pair_in[...].astype(F32)
    share = pairs // n
    odd = lax.rem(row, 2)
    for chip in range(n):
        rows = slice(chip * share, chip * share + share)
        block = jnp.concatenate([value[rows, :pairs], value[rows, pairs:]], axis=0)
        place = (chip % 2, chip // 2 % 2, chip // 4)
        own_sums[place] = block
        near_out[place] = block.astype(BF16)

    def near_copy(way):
        step = lax.rem(odd + way, 2) * -2 + 1
        return pltpu.make_async_remote_copy(
            src_ref=near_out.at[1 - odd, way],
            dst_ref=near_in.at[way],
            send_sem=near_send.at[way],
            recv_sem=near_recv.at[way],
            device_id={"row": lax.rem(row + step + n, n)},
            device_id_type=MESH,
        )

    def far_copy(to_row, from_row, target):
        return pltpu.make_async_remote_copy(
            src_ref=far_out.at[lax.rem(to_row // 2, 2), to_row // 4],
            dst_ref=far_in.at[from_row // 2],
            send_sem=far_send.at[to_row // 2],
            recv_sem=far_recv.at[from_row // 2],
            device_id={"row": target},
            device_id_type=MESH,
        )

    for way in range(2):
        near_copy(way).start()
    for way in range(2):
        near_copy(way).wait()
        both = own_sums[odd, way] + near_in[way].astype(F32)
        own_sums[odd, way] = both
        far_out[way] = both.astype(BF16)
    chips = n // 2
    for offset in range(chips - 1):
        away = chips // 2 + (offset + 1) // 2 * (1 if offset % 2 else -1)
        target = lax.rem(row + 2 * away, n)
        far_copy(target, row, target).start()
    total = own_sums[odd, lax.rem(row // 2, 2), row // 4]
    for offset in range(chips - 1):
        away = 1 + offset // 2 if offset % 2 == 0 else chips - 1 - offset // 2
        source = lax.rem(row + 2 * away, n)
        far_copy(source, source, source).wait_recv()
        total = total + far_in[source // 2].astype(F32)
    for away in range(1, chips):
        target = lax.rem(row + 2 * away, n)
        far_copy(target, row, target).wait_send()
    part = share // 2
    pieces = [jnp.stack([total[c * part : c * part + part], total[share + c * part : share + c * part + part]]) for c in range(2)]
    is_first = col == 0
    last_out[...] = jnp.where(is_first, pieces[1], pieces[0])
    last_copy = pltpu.make_async_remote_copy(
        src_ref=last_out, dst_ref=last_in, send_sem=last_sems.at[0], recv_sem=last_sems.at[1],
        device_id={"col": 1 - col}, device_id_type=MESH,
    )
    last_copy.start()
    out_ref[col] = jnp.where(is_first, pieces[0], pieces[1])
    last_copy.wait()
    out_ref[1 - col] = last_in[...]


VMEM = pl.BlockSpec(memory_space=pltpu.VMEM)
DMA = pltpu.SemaphoreType.DMA


def shards(n, wannier, pairs, gmap, screened):
    members, planes, cells = wannier.shape
    count = pairs.shape[0]
    depth = cells // 4
    halves = n // 2
    waves = gmap.shape[0] // (2 * n)
    rho = pl.pallas_call(
        functools.partial(wave_kernel, n),
        out_shape=jax.ShapeDtypeStruct((2 * waves, count), BF16),
        in_specs=[VMEM] * 3,
        out_specs=VMEM,
        scratch_shapes=[
            pltpu.VMEM((depth, 4 * members), BF16),
            pltpu.VMEM((waves, 128), jnp.int32),
            pltpu.VMEM((2 * n, depth, 4 * members), BF16),
            pltpu.VMEM((waves, cells // 2), BF16),
            pltpu.VMEM((waves, cells // 2), BF16),
            pltpu.VMEM((6, waves, 128), F32),
            pltpu.VMEM((6, waves, 128), F32),
        ]
        + [pltpu.VMEM((cells // 2, 2 * count), BF16)] * 4
        + [pltpu.VMEM((waves, count), F32)] * 2
        + [DMA((2, 2, halves)), DMA((2, 2, halves)), DMA((n,)), DMA((n,))],
        compiler_params=pltpu.CompilerParams(collective_id=0, has_side_effects=True),
        name="waves",
    )(wannier, pairs.T, gmap.reshape(-1, 128))

    freqs, _, row_span, col_span = screened.shape
    share = count // n
    return pl.pallas_call(
        functools.partial(matrix_kernel, n, 1.0 / math.sqrt(gmap.shape[0])),
        out_shape=jax.ShapeDtypeStruct((freqs, 2, share // 2, count), F32),
        in_specs=[VMEM, pl.BlockSpec(memory_space=pl.ANY)],
        out_specs=VMEM,
        scratch_shapes=[
            pltpu.VMEM((n, 2 * waves, count), BF16),
            pltpu.VMEM(screened.shape, BF16),
            pltpu.VMEM((freqs, row_span, 2 * count), F32),
            pltpu.VMEM((row_span // waves, 2 * waves, count), BF16),
            pltpu.VMEM((count, 2 * count), BF16),
            pltpu.VMEM((count, 2 * count), BF16),
            pltpu.VMEM((2, 2, n // 4, 2 * share, count), F32),
            pltpu.VMEM((2, 2, n // 4, 2 * share, count), BF16),
            pltpu.VMEM((2, n // 4, 2 * share, count), BF16),
            pltpu.VMEM((2, n // 4, 2 * share, count), BF16),
            pltpu.VMEM((n // 2, 2 * share, count), BF16),
            pltpu.VMEM((2, share // 2, count), F32),
            pltpu.VMEM((2, share // 2, count), F32),
            DMA((2, 2)),
            DMA((2, 2, halves)),
            DMA((2, 2, halves)),
            DMA((row_span // waves,)),
            DMA((row_span // waves,)),
            DMA((2,)),
            DMA((2,)),
            DMA((2,)),
            DMA((halves,)),
            DMA((halves,)),
            DMA((2,)),
        ],
        compiler_params=pltpu.CompilerParams(collective_id=1, has_side_effects=True, vmem_limit_bytes=60 << 20),
        name="matrix",
    )(rho, screened)


def solution(mesh):
    return jax.shard_map(
        functools.partial(shards, mesh.shape["row"]),
        mesh=mesh,
        in_specs=(P("kpt", ("row", "col"), None), P(), P(), P("kpt", None, "row", "col")),
        out_specs=P(None, None, ("kpt", "row", "col"), None),
        check_vma=False,
    )
```

```python
import functools
import math

import jax
import jax.numpy as jnp
from jax import lax
from jax.experimental import pallas as pl
from jax.experimental.pallas import tpu as pltpu
from jax.sharding import PartitionSpec as P

MESH = pl.DeviceIdType.MESH
GX = 32
F32 = jnp.float32
BF16 = jnp.bfloat16


def dot(a, b):
    return lax.dot_general(a, b, (((1,), (0,)), ((), ())), preferred_element_type=F32)


def dot_tn(a, b):
    return lax.dot_general(a, b, (((0,), (0,)), ((), ())), preferred_element_type=F32)


def greet(targets, between=None):
    barrier = pltpu.get_barrier_semaphore()
    for target in targets:
        pl.semaphore_signal(barrier, inc=1, device_id=target, device_id_type=MESH)
    if between is not None:
        between()
    pl.semaphore_wait(barrier, len(targets))


class Ring:
    def __init__(self, n, own_ref, slot_ref, send_sems, recv_sems):
        self.n, self.half = n, n // 2
        self.own, self.slot = own_ref, slot_ref
        self.send_sems, self.recv_sems = send_sems, recv_sems
        self.me = lax.axis_index("row")
        self.rows = own_ref.shape[0] // 2

    def owner(self, way, step):
        return lax.rem(self.me + step + self.n, self.n) if way else lax.rem(self.me - step + self.n, self.n)

    def copy(self, way, chunk, step, first, arriving=False):
        span = pl.ds(chunk * self.rows, self.rows)
        place = self.slot(self.owner(way, step + 1 if arriving else step)).at[span]
        source = self.own.at[span] if first else place
        target = self.owner(way, -1)
        return pltpu.make_async_remote_copy(
            src_ref=source,
            dst_ref=place,
            send_sem=self.send_sems.at[way, chunk, step],
            recv_sem=self.recv_sems.at[way, chunk, step],
            device_id={"row": self.owner(1 - way, 1)},
            device_id_type=MESH,
        )

    def run(self, on_block, before=None):
        last = self.half - 1
        for way in range(2):
            for chunk in range(2):
                self.copy(way, chunk, 0, True).start()
        if before is not None:
            before()

        def forward(chunk, step, ways):
            for way in range(2):
                self.copy(way, chunk, step - 1, False, True).wait_recv()
                if way in ways:
                    self.copy(way, chunk, step, False).start()

        for chunk in range(2):
            forward(chunk, 1, (0, 1))

        def step_body(step, _):
            for chunk in range(2):
                forward(chunk, step, (0, 1))
                on_block(self.owner(chunk, step - 1))
            return 0

        lax.fori_loop(2, last, step_body, 0)
        for chunk in range(2):
            forward(chunk, last, (chunk,))
            on_block(self.owner(chunk, last - 1))
        on_block(self.owner(0, last))
        on_block(self.owner(1, last))
        for way in range(2):
            self.copy(way, way, last, False, True).wait_recv()
        on_block(self.owner(0, self.half))

    def drain(self):
        for way in range(2):
            for chunk in range(2):
                self.copy(way, chunk, 0, True).wait_send()

        def body(step, _):
            for way in range(2):
                for chunk in range(2):
                    self.copy(way, chunk, step, False).wait_send()
            return 0

        lax.fori_loop(1, self.half - 1, body, 0)
        for way in range(2):
            self.copy(way, way, self.half - 1, False).wait_send()


def neighbours(n, cols):
    row, col = lax.axis_index("row"), lax.axis_index("col")
    right, left = lax.rem(row + 1, n), lax.rem(row + n - 1, n)
    return [{"row": right}, {"row": left}, {"col": 1 - col}]


def pick_lanes(values, lanes):
    numbers = lax.GatherDimensionNumbers(
        offset_dims=(), collapsed_slice_dims=(1,), start_index_map=(1,), operand_batching_dims=(0,), start_indices_batching_dims=(0,)
    )
    return lax.gather(values, lanes[:, :, None], numbers, (1, 1), mode=lax.GatherScatterMode.PROMISE_IN_BOUNDS)


def wave_kernel(
    n, wannier_ref, pick_ref, gmap_ref, out_ref, own_ref, cell_ref, planes, cosine, sine, turn, power, even0, odd0, even1, odd1, acc_re, acc_im,
    send_sems, recv_sems, pair_send, pair_recv,
):
    row, col = lax.axis_index("row"), lax.axis_index("col")
    depth = own_ref.shape[0]
    waves, pairs = acc_re.shape
    tiles = pairs // 128
    piece = 64

    def prepare():
        values = wannier_ref[:, 0, :]
        back = 127 - lax.broadcasted_iota(jnp.int32, (values.shape[0], 128), 1)
        parts = [values[:, :depth], values[:, depth : 2 * depth]]
        for quarter in (3, 2):
            tail = [pick_lanes(values[:, quarter * depth + lane : quarter * depth + lane + 128], back) for lane in range(0, depth, 128)]
            parts.append(jnp.concatenate(tail[::-1], axis=1))
        own_ref[...] = jnp.concatenate(parts, axis=0).T.astype(BF16)
        for begin in range(0, waves, 128):
            line = gmap_ref[pl.ds((col * n + row) * (waves // 128) + begin // 128, 1), :].astype(F32)
            cell_ref[pl.ds(begin, 128)] = jnp.broadcast_to(line, (128, 128)).T.astype(jnp.int32)

    greet(neighbours(n, 2), prepare)

    def slot(owner, which):
        return planes.at[owner * 2 + which]

    def pair_copy(source, owner, to_col):
        return pltpu.make_async_remote_copy(
            src_ref=source,
            dst_ref=slot(owner, to_col),
            send_sem=pair_send.at[owner],
            recv_sem=pair_recv.at[owner],
            device_id={"col": 1 - col},
            device_id_type=MESH,
        )

    def fold(owner, tile, even, odd):
        for which in range(2):
            columns = pl.ds(pl.multiple_of(tile * 256 + which * 128, 128), 128)
            for begin in range(0, depth, piece):
                plane = planes[owner * 2 + which, pl.ds(begin, piece)].astype(F32)
                for part in range(2):
                    values = []
                    for quarter in (part, part + 2):
                        for side in range(2):
                            lanes = pick_ref[pl.ds(side, 1), pl.ds(pl.multiple_of(tile * 128, 128), 128)] + quarter * 32
                            values.append(pick_lanes(plane, jnp.broadcast_to(lanes, plane.shape)))
                    one, two = values[0] * values[1], values[2] * values[3]
                    span = pl.ds(part * depth + begin, piece)
                    even[span, columns] = (one + two).astype(BF16)
                    odd[span, columns] = (one - two).astype(BF16)

    def gather(tile, even, odd, sign):
        columns = pl.ds(pl.multiple_of(tile * 128, 128), 128)
        block = pl.ds(pl.multiple_of(tile * 256, 256), 256)
        real = dot(cosine[...], even[:, block])
        imag = dot(sine[...], odd[:, block])
        p_re, p_im = power[0], power[1] * sign
        at = 2 if sign > 0 else 4
        q_re, q_im = power[at], power[at + 1]
        acc_re[:, columns] += p_re * real[:, :128] - p_im * imag[:, :128] + (q_re * real[:, 128:] - q_im * imag[:, 128:])
        acc_im[:, columns] += p_re * imag[:, :128] + p_im * real[:, :128] + (q_re * imag[:, 128:] + q_im * real[:, 128:])

    def set_power(p_re, p_im):
        power[0], power[1] = p_re, p_im
        one, two = p_re * turn[0], p_im * turn[1]
        three, four = p_re * turn[1], p_im * turn[0]
        power[2], power[3] = one - two, three + four
        power[4], power[5] = one + two, three - four

    def tables():
        lane = lax.broadcasted_iota(jnp.int32, (8, 128), 1)
        angle = (lane & (2 * GX - 1)).astype(F32) * (math.pi / GX)
        cos_lanes, sin_lanes = jnp.cos(angle), jnp.sin(angle)
        copies = waves // 8

        def look(steps):
            at = steps & (2 * GX - 1)
            return (
                pick_lanes(jnp.concatenate([cos_lanes] * copies, axis=0), at),
                pick_lanes(jnp.concatenate([sin_lanes] * copies, axis=0), at),
            )

        bits = GX.bit_length() - 1
        cell = cell_ref[...]
        kx, ky, kz = cell >> (2 * bits), (cell >> bits) & (GX - 1), cell & (GX - 1)

        def fill(index, _):
            begin = pl.multiple_of(index * 128, 128)
            spot = lax.broadcasted_iota(jnp.int32, cell.shape, 1) + begin
            real, imag = look(ky * (2 * (spot >> bits) + 1) + kz * (2 * (spot & (GX - 1)) + 1))
            cosine[:, pl.ds(begin, 128)] = real.astype(BF16)
            sine[:, pl.ds(begin, 128)] = (-imag).astype(BF16)
            return 0

        lax.fori_loop(0, 2 * depth // 128, fill, 0)
        turn[0], turn[1] = look(kx * -2)
        turn[2], turn[3] = look(kx * -4)
        norm = 1.0 / math.sqrt(GX * GX * GX)
        real, imag = look(ky + kz - kx * 4 * row)
        turn[4], turn[5] = real * norm, imag * norm
        set_power(jnp.ones(cell.shape, F32), jnp.zeros(cell.shape, F32))

    def advance():
        p_re, p_im = power[0], power[1]
        set_power(p_re * turn[2] - p_im * turn[3], p_re * turn[3] + p_im * turn[2])

    ring = Ring(n, own_ref, lambda owner: slot(owner, col), send_sems, recv_sems)
    half = n // 2

    def arrive(step):
        for chunk in range(2):
            for way in range(2):
                if way == chunk:
                    ring.copy(way, chunk, step - 1, False, True).wait_recv()

                    @pl.when(step < half)
                    def _():
                        ring.copy(way, chunk, step, False).start()
                else:
                    @pl.when(step < half)
                    def _():
                        ring.copy(way, chunk, step - 1, False, True).wait_recv()

                    @pl.when(step < half - 1)
                    def _():
                        ring.copy(way, chunk, step, False).start()
        ahead, behind = ring.owner(1, step), ring.owner(0, step)
        pair_copy(slot(ahead, col), ahead, col).start()

        @pl.when(step < half)
        def _():
            pair_copy(slot(behind, col), behind, col).start()

    def paired(owner):
        pair_copy(own_ref, owner, 1 - col).wait_recv()

    def each_tile(work):
        def one(tile, _):
            work(tile)
            return 0

        lax.fori_loop(0, tiles, one, 0)

    def first_half(owner):
        def work(tile):
            gather(tile, even1, odd1, -1.0)
            fold(owner, tile, even0, odd0)

        each_tile(work)
        advance()

    for way in range(2):
        for chunk in range(2):
            ring.copy(way, chunk, 0, True).start()
    pair_copy(own_ref, row, col).start()
    planes[row * 2 + col] = own_ref[...]
    acc_re[...] = jnp.zeros_like(acc_re)
    acc_im[...] = jnp.zeros_like(acc_im)
    tables()
    arrive(1)
    paired(row)
    each_tile(lambda tile: fold(row, tile, even1, odd1))

    def body(step, _):
        arrive(step)
        ahead, behind = ring.owner(1, step - 1), ring.owner(0, step - 1)
        paired(ahead)
        paired(behind)
        first_half(ahead)

        def work(tile):
            gather(tile, even0, odd0, 1.0)
            fold(behind, tile, even1, odd1)

        each_tile(work)
        return 0

    lax.fori_loop(2, half + 1, body, 0)
    across = ring.owner(0, half)
    paired(across)
    first_half(across)
    each_tile(lambda tile: gather(tile, even0, odd0, 1.0))
    for tile in range(tiles):
        columns = pl.ds(tile * 128, 128)
        real, imag = acc_re[:, columns], acc_im[:, columns]
        out_ref[pl.ds(0, waves), columns] = (real * turn[4] - imag * turn[5]).astype(BF16)
        out_ref[pl.ds(waves, waves), columns] = (real * turn[5] + imag * turn[4]).astype(BF16)
    ring.drain()

    def finish(owner, _):
        pair_copy(own_ref, owner, col).wait_send()
        return 0

    lax.fori_loop(0, n, finish, 0)


def matrix_kernel(
    n, scale, rho_ref, w_hbm, out_ref, panel, w_vmem, mixed, left, pair_out, pair_in, own_sums, near_out, near_in,
    far_out, far_in, last_out, last_in, w_sems, send_sems, recv_sems, left_send, left_recv, pair_sems, near_send, near_recv,
    far_send, far_recv, last_sems,
):
    row, col = lax.axis_index("row"), lax.axis_index("col")
    waves, pairs = rho_ref.shape[0] // 2, rho_ref.shape[1]
    span = mixed.shape[1]
    per_row = span // waves
    owner_col = row // (n // 2)
    holds_left = col == owner_col
    base = lax.rem(row, n // 2) * per_row
    loads = [pltpu.make_async_copy(w_hbm.at[f, part], w_vmem.at[f, part], w_sems.at[f, part]) for f in range(2) for part in range(2)]
    for load in loads:
        load.start()
    greet(neighbours(n, 2))

    def left_copy(owner, place):
        return pltpu.make_async_remote_copy(
            src_ref=panel.at[owner],
            dst_ref=left.at[place],
            send_sem=left_send.at[place],
            recv_sem=left_recv.at[place],
            device_id={"col": 1 - col},
            device_id_type=MESH,
        )

    def multiply(owner, fresh=False):
        columns = pl.ds(pl.multiple_of(owner * waves, waves), waves)
        real, imag = panel[owner, pl.ds(0, waves)], panel[owner, pl.ds(waves, waves)]
        first = jnp.concatenate([real, imag], axis=1)
        second = jnp.concatenate([-imag, real], axis=1)

        def one(f, _):
            value = dot(w_vmem[f, 0, :, columns], first) + dot(w_vmem[f, 1, :, columns], second)
            mixed[f] = value if fresh else mixed[f] + value
            return 0

        lax.fori_loop(0, 2, one, 0)

    def on_block(owner):
        @pl.when(holds_left & (owner >= base) & (owner < base + per_row))
        def _():
            left_copy(owner, owner - base).start()

        multiply(owner)

    def before():
        panel[row] = rho_ref[...]

        @pl.when(holds_left & (row >= base) & (row < base + per_row))
        def _():
            left_copy(row, row - base).start()

        for load in loads:
            load.wait()
        multiply(row, True)

    ring = Ring(n, rho_ref, lambda owner: panel.at[owner], send_sems, recv_sems)
    ring.run(on_block, before)

    @pl.when(holds_left)
    def _():
        for place in range(per_row):
            left_copy(base + place, place).wait_send()
            left[place] = panel[base + place]

    @pl.when(jnp.logical_not(holds_left))
    def _():
        for place in range(per_row):
            left_copy(base + place, place).wait_recv()

    def elements(f):
        total = None
        for place in range(per_row):
            rows = pl.ds(place * waves, waves)
            real = mixed[f, rows, pl.ds(0, pairs)].astype(BF16)
            imag = mixed[f, rows, pl.ds(pairs, pairs)].astype(BF16)
            one = dot_tn(left[place, pl.ds(0, waves)], jnp.concatenate([real, imag], axis=1))
            two = dot_tn(left[place, pl.ds(waves, waves)], jnp.concatenate([imag, -real], axis=1))
            total = one + two if total is None else total + one + two
        return total * scale

    pair_copy = pltpu.make_async_remote_copy(
        src_ref=pair_out, dst_ref=pair_in, send_sem=pair_sems.at[0], recv_sem=pair_sems.at[1],
        device_id={"col": 1 - col}, device_id_type=MESH,
    )
    pair_out[...] = elements(1 - col).astype(BF16)
    pair_copy.start()
    value = elements(col)
    ring.drain()
    pair_copy.wait()
    value = value + pair_in[...].astype(F32)
    share = pairs // n
    odd = lax.rem(row, 2)
    for chip in range(n):
        rows = slice(chip * share, chip * share + share)
        block = jnp.concatenate([value[rows, :pairs], value[rows, pairs:]], axis=0)
        place = (chip % 2, chip // 2 % 2, chip // 4)
        own_sums[place] = block
        near_out[place] = block.astype(BF16)

    def near_copy(way):
        step = lax.rem(odd + way, 2) * -2 + 1
        return pltpu.make_async_remote_copy(
            src_ref=near_out.at[1 - odd, way],
            dst_ref=near_in.at[way],
            send_sem=near_send.at[way],
            recv_sem=near_recv.at[way],
            device_id={"row": lax.rem(row + step + n, n)},
            device_id_type=MESH,
        )

    def far_copy(to_row, from_row, target):
        return pltpu.make_async_remote_copy(
            src_ref=far_out.at[lax.rem(to_row // 2, 2), to_row // 4],
            dst_ref=far_in.at[from_row // 2],
            send_sem=far_send.at[to_row // 2],
            recv_sem=far_recv.at[from_row // 2],
            device_id={"row": target},
            device_id_type=MESH,
        )

    for way in range(2):
        near_copy(way).start()
    for way in range(2):
        near_copy(way).wait()
        both = own_sums[odd, way] + near_in[way].astype(F32)
        own_sums[odd, way] = both
        far_out[way] = both.astype(BF16)
    chips = n // 2
    for offset in range(chips - 1):
        away = chips // 2 + (offset + 1) // 2 * (1 if offset % 2 else -1)
        target = lax.rem(row + 2 * away, n)
        far_copy(target, row, target).start()
    total = own_sums[odd, lax.rem(row // 2, 2), row // 4]
    for offset in range(chips - 1):
        away = 1 + offset // 2 if offset % 2 == 0 else chips - 1 - offset // 2
        source = lax.rem(row + 2 * away, n)
        far_copy(source, source, source).wait_recv()
        total = total + far_in[source // 2].astype(F32)
    for away in range(1, chips):
        target = lax.rem(row + 2 * away, n)
        far_copy(target, row, target).wait_send()
    part = share // 2
    pieces = [jnp.stack([total[c * part : c * part + part], total[share + c * part : share + c * part + part]]) for c in range(2)]
    is_first = col == 0
    last_out[...] = jnp.where(is_first, pieces[1], pieces[0])
    last_copy = pltpu.make_async_remote_copy(
        src_ref=last_out, dst_ref=last_in, send_sem=last_sems.at[0], recv_sem=last_sems.at[1],
        device_id={"col": 1 - col}, device_id_type=MESH,
    )
    last_copy.start()
    out_ref[col] = jnp.where(is_first, pieces[0], pieces[1])
    last_copy.wait()
    out_ref[1 - col] = last_in[...]


VMEM = pl.BlockSpec(memory_space=pltpu.VMEM)
DMA = pltpu.SemaphoreType.DMA


def shards(n, wannier, pairs, gmap, screened):
    members, planes, cells = wannier.shape
    count = pairs.shape[0]
    depth = cells // 4
    halves = n // 2
    waves = gmap.shape[0] // (2 * n)
    rho = pl.pallas_call(
        functools.partial(wave_kernel, n),
        out_shape=jax.ShapeDtypeStruct((2 * waves, count), BF16),
        in_specs=[VMEM] * 3,
        out_specs=VMEM,
        scratch_shapes=[
            pltpu.VMEM((depth, 4 * members), BF16),
            pltpu.VMEM((waves, 128), jnp.int32),
            pltpu.VMEM((2 * n, depth, 4 * members), BF16),
            pltpu.VMEM((waves, cells // 2), BF16),
            pltpu.VMEM((waves, cells // 2), BF16),
            pltpu.VMEM((6, waves, 128), F32),
            pltpu.VMEM((6, waves, 128), F32),
        ]
        + [pltpu.VMEM((cells // 2, 2 * count), BF16)] * 4
        + [pltpu.VMEM((waves, count), F32)] * 2
        + [DMA((2, 2, halves)), DMA((2, 2, halves)), DMA((n,)), DMA((n,))],
        compiler_params=pltpu.CompilerParams(collective_id=0, has_side_effects=True),
        name="waves",
    )(wannier, pairs.T, gmap.reshape(-1, 128))

    freqs, _, row_span, col_span = screened.shape
    share = count // n
    return pl.pallas_call(
        functools.partial(matrix_kernel, n, 1.0 / math.sqrt(gmap.shape[0])),
        out_shape=jax.ShapeDtypeStruct((freqs, 2, share // 2, count), F32),
        in_specs=[VMEM, pl.BlockSpec(memory_space=pl.ANY)],
        out_specs=VMEM,
        scratch_shapes=[
            pltpu.VMEM((n, 2 * waves, count), BF16),
            pltpu.VMEM(screened.shape, BF16),
            pltpu.VMEM((freqs, row_span, 2 * count), F32),
            pltpu.VMEM((row_span // waves, 2 * waves, count), BF16),
            pltpu.VMEM((count, 2 * count), BF16),
            pltpu.VMEM((count, 2 * count), BF16),
            pltpu.VMEM((2, 2, n // 4, 2 * share, count), F32),
            pltpu.VMEM((2, 2, n // 4, 2 * share, count), BF16),
            pltpu.VMEM((2, n // 4, 2 * share, count), BF16),
            pltpu.VMEM((2, n // 4, 2 * share, count), BF16),
            pltpu.VMEM((n // 2, 2 * share, count), BF16),
            pltpu.VMEM((2, share // 2, count), F32),
            pltpu.VMEM((2, share // 2, count), F32),
            DMA((2, 2)),
            DMA((2, 2, halves)),
            DMA((2, 2, halves)),
            DMA((row_span // waves,)),
            DMA((row_span // waves,)),
            DMA((2,)),
            DMA((2,)),
            DMA((2,)),
            DMA((halves,)),
            DMA((halves,)),
            DMA((2,)),
        ],
        compiler_params=pltpu.CompilerParams(collective_id=1, has_side_effects=True, vmem_limit_bytes=60 << 20),
        name="matrix",
    )(rho, screened)


def solution(mesh):
    return jax.shard_map(
        functools.partial(shards, mesh.shape["row"]),
        mesh=mesh,
        in_specs=(P("kpt", ("row", "col"), None), P(), P(), P("kpt", None, "row", "col")),
        out_specs=P(None, None, ("kpt", "row", "col"), None),
        check_vma=False,
    )
```
